128 devices in a mesh: blk: 16 (over z, x_hi, core), uly: 8 (over y, x_lo).
Axes of the slice: x: 4 (x_hi: 2, x_lo: 2; x = x_hi * 2 + x_lo), y: 4, z: 4, core: 2. Of those that a mesh axis runs over, the one named last changes fastest.
Arguments:
- queries: bfloat16 [2048, 128, 128], P(('blk', 'uly')), may hold values from -8 to 8
- query_tangents: bfloat16 [2048, 128, 4, 128], P(('blk', 'uly')), may hold values from -6 to 6
- keys: bfloat16 [2048, 8, 128], P(('blk', 'uly')), may hold values from -8 to 8
- key_tangents: bfloat16 [2048, 8, 4, 128], P(('blk', 'uly')), may hold values from -6 to 6
- values: bfloat16 [2048, 8, 128], P(('blk', 'uly')), may hold values from -6 to 6
- value_tangents: bfloat16 [2048, 8, 4, 128], P(('blk', 'uly')), may hold values from -6 to 6
- span_order: int32 [32], replicated, may hold values from 0 to 31, as said below
Outputs:
- attention_out: bfloat16 [2048, 128, 128], P(('blk', 'uly'))
- tangent_out: bfloat16 [2048, 128, 4, 128], P(('blk', 'uly'))
The draws below stay inside these ranges and needn't reach their ends.
Inputs may be any that keep to these rules, and one draw needn't show every extreme that they name: span_order is a permutation of the span positions; for every b the stored spans 2 * b and 2 * b + 1 hold positions c and 31 - c for some c.
All inputs are finite; a program needn't handle non-finite values.
Results may differ from the reference program's by a relative error of at most 0.0055.
Values may be sent and summed in bfloat16 or wider, within the bound.
No kernel may reach another device: no remote copies, remote signals or barrier semaphores. Data moves between devices by JAX's collectives and lax.ppermute only.
A program may use at most 64 MiB of HBM per device.

```python
import jax
import jax.numpy as jnp
from jax import lax

HD = 128
HQ = 128
KVH = 8
P_SIZE = 4
SEQ_DEV = 128
SEQ = 2048
SPAN = 64
SPANS = 32


def drawn_pair(key):
    query_key = jax.random.fold_in(key, 11)
    keys_key = jax.random.fold_in(key, 12)
    queries = jax.random.truncated_normal(query_key, -4.0, 4.0, (SEQ, HQ, HD), jnp.float32)
    keyset = jax.random.truncated_normal(keys_key, -4.0, 4.0, (SEQ, KVH, HD), jnp.float32)
    return (queries, keyset)


def draw_queries(key, part):
    return drawn_pair(key)[0].astype(jnp.bfloat16)


def draw_keys(key, part):
    return drawn_pair(key)[1].astype(jnp.bfloat16)


def draw_span_order(key, part):
    pairs = SPANS // 2
    chosen = jax.random.permutation(jax.random.fold_in(key, 21), pairs).astype(jnp.int32)
    flipped = jax.random.randint(jax.random.fold_in(key, 22), (pairs,), 0, 2, jnp.int32)
    first = jnp.where(flipped == 1, chosen, SPANS - 1 - chosen)
    second = SPANS - 1 - first
    return jnp.stack([first, second], axis=1).reshape(SPANS).astype(jnp.int32)


def block_levels(stream_key, dims, pieces, least, high):
    factor_of, own = 1.0, jax.random.fold_in(stream_key, 6)
    for dim, blocks in pieces:
        heights = jnp.exp(jax.random.uniform(jax.random.fold_in(own, dim), (blocks,), jnp.float32, least / len(pieces), high / len(pieces)))
        factor_of = factor_of * jnp.repeat(heights, dims[dim] // blocks).reshape([-1 if axis == dim else 1 for axis in range(len(dims))])
    return factor_of


def bell_draw(stream_key, extent, deviation, limit, shards=(), kind=jnp.bfloat16):
    drawn = deviation * jax.random.normal(stream_key, extent, jnp.float32)
    if shards:
        drawn = drawn * block_levels(stream_key, extent, shards, -0.22, 0.18)
    return jnp.clip(drawn, -limit, limit).astype(kind)


def setup_inputs(seed: int = 0) -> dict:
    key_of = jax.random.split(jax.random.key(seed), 8)
    return {
        "queries": draw_queries(jax.random.fold_in(key_of[7], 71), 0),
        "query_tangents": bell_draw(key_of[1], (SEQ, HQ, P_SIZE, HD), 1.0, 6.0, ((0, 128),)),
        "keys": draw_keys(jax.random.fold_in(key_of[7], 71), 0),
        "key_tangents": bell_draw(key_of[3], (SEQ, KVH, P_SIZE, HD), 1.0, 6.0, ((0, 128),)),
        "values": bell_draw(key_of[4], (SEQ, KVH, HD), 1.0, 6.0, ((0, 128),)),
        "value_tangents": bell_draw(key_of[5], (SEQ, KVH, P_SIZE, HD), 1.0, 6.0, ((0, 128),)),
        "span_order": draw_span_order(jax.random.fold_in(key_of[7], 71), 0),
    }


def reference(queries, query_tangents, keys, key_tangents, values, value_tangents, span_order):
    stored = jnp.arange(SEQ, dtype=jnp.int32)
    position = (span_order[stored // SPAN] * SPAN + stored % SPAN).astype(jnp.int32)
    scaling = HD ** -0.5
    group = HQ // KVH
    block_rows = SEQ_DEV
    block_total = SEQ // block_rows
    keys_wide = keys.astype(jnp.float32)
    key_tan_wide = key_tangents.astype(jnp.float32)
    values_wide = values.astype(jnp.float32)
    value_tan_wide = value_tangents.astype(jnp.float32)
    highest = lax.Precision.HIGHEST

    def one_block(index):
        head = (index // block_total).astype(jnp.int32)
        kv_head = (head // group).astype(jnp.int32)
        begin = ((index % block_total) * block_rows).astype(jnp.int32)
        zero = jnp.zeros((), jnp.int32)
        query_block = lax.dynamic_slice(queries, (begin, head, zero), (block_rows, 1, HD))[:, 0]
        tangent_block = lax.dynamic_slice(query_tangents, (begin, head, zero, zero), (block_rows, 1, P_SIZE, HD))[:, 0]
        key_half = lax.dynamic_index_in_dim(keys, kv_head, 1, keepdims=False)
        value_half = lax.dynamic_index_in_dim(values, kv_head, 1, keepdims=False)
        key_f = lax.dynamic_index_in_dim(keys_wide, kv_head, 1, keepdims=False)
        key_tan_f = lax.dynamic_index_in_dim(key_tan_wide, kv_head, 1, keepdims=False)
        value_f = lax.dynamic_index_in_dim(values_wide, kv_head, 1, keepdims=False)
        value_tan_f = lax.dynamic_index_in_dim(value_tan_wide, kv_head, 1, keepdims=False)
        query_places = lax.dynamic_slice_in_dim(position, begin, block_rows)
        scores = jnp.dot(query_block, key_half.T, preferred_element_type=jnp.float32) * scaling
        visible = position[None, :] <= query_places[:, None]
        scores = jnp.where(visible, scores, -1e30)
        top = jnp.max(scores, axis=1, keepdims=True)
        weights_full = jnp.where(visible, jnp.exp(scores - top), 0.0)
        total = jnp.sum(weights_full, axis=1)
        weights = weights_full.astype(jnp.bfloat16)
        score_tan = jnp.einsum("qpd,kd->pqk", tangent_block.astype(jnp.float32), key_f, precision=highest)
        score_tan = score_tan + jnp.einsum("qd,kpd->pqk", query_block.astype(jnp.float32), key_tan_f, precision=highest)
        score_tan = score_tan * scaling
        weighted = weights_full[None] * score_tan
        shift = jnp.sum(weighted, axis=2)
        weighted_half = weighted.astype(jnp.bfloat16)
        primal_sum = jnp.dot(weights, value_half, preferred_element_type=jnp.float32)
        tangent_sum = jnp.einsum("pqk,kd->pqd", weighted_half.astype(jnp.float32), value_f, precision=highest)
        tangent_sum = tangent_sum + jnp.einsum("qk,kpd->pqd", weights.astype(jnp.float32), value_tan_f, precision=highest)
        primal = primal_sum / total[:, None]
        tangent = tangent_sum / total[None, :, None] - primal[None] * (shift / total[None])[..., None]
        return primal.astype(jnp.bfloat16), tangent.astype(jnp.bfloat16)

    outputs, tangents = lax.map(one_block, jnp.arange(HQ * block_total, dtype=jnp.int32))
    outputs = outputs.reshape(HQ, block_total, block_rows, HD).transpose(1, 2, 0, 3).reshape(SEQ, HQ, HD)
    tangents = tangents.reshape(HQ, block_total, P_SIZE, block_rows, HD).transpose(1, 3, 0, 2, 4).reshape(SEQ, HQ, P_SIZE, HD)
    return outputs, tangents
```

```python
import functools
import math

import jax
import jax.numpy as jnp
from jax import lax
from jax.experimental import pallas as pl
from jax.experimental.pallas import tpu as pltpu
from jax.sharding import PartitionSpec as P

HD = 128
HQ = 128
KVH = 8
P_SIZE = 4
GROUP = HQ // KVH
SPAN = 64
SPANS = 32
ULY = 8
ROWS = 16
KB = 256
PER_BLOCK = KB // SPAN
BLOCKS = SPANS // PER_BLOCK
TILE = 512
HALF = SPAN * GROUP
WIDTH = HD * (2 + 2 * P_SIZE)
SCALE = HD**-0.5
LOG2E = math.log2(math.e)
F32 = jnp.float32
BF16 = jnp.bfloat16


def over_last(a, b):
    return lax.dot_general(a, b, (((1,), (1,)), ((), ())), preferred_element_type=F32)


def attend(meta, x_ref, kv_hbm, out_ref, kv, scores, top, acc, sems):
    first = 2 * meta[SPANS]
    limit = jnp.maximum(meta[first], meta[first + 1])

    def copy_of(j):
        at = pl.multiple_of(meta[j] * SPAN, SPAN)
        return pltpu.make_async_copy(
            kv_hbm.at[pl.ds(j * SPAN, SPAN), :], kv.at[pl.ds(at, SPAN), :], sems.at[j]
        )

    for j in range(SPANS):
        copy_of(j).start()
    for j in range(SPANS):
        copy_of(j).wait()

    ones = jnp.ones((KB, HD), BF16)

    def tile(index, unused):
        half = index // (HALF // TILE)
        part = index % (HALF // TILE)
        pos = meta[first + half]
        blocks = pos // PER_BLOCK + 1
        sources = TILE // 256
        source = half * 4 + part * sources

        def rows_of(k):
            return x_ref[pl.ds(source, sources), k].reshape(TILE, HD)

        def score(b):
            at = pl.multiple_of(b * KB, KB)
            return over_last(rows_of(0), kv[pl.ds(at, KB), 0:HD])

        def keep(b, s):
            scores[b] = s
            top[...] = jnp.maximum(top[...], jnp.maximum(s[:, :HD], s[:, HD:]))

        top[...] = jnp.full((TILE, HD), -1e30, F32)

        def first_pass(b, carry):
            keep(b, score(b))
            return carry

        lax.fori_loop(0, blocks - 1, first_pass, 0)
        last = blocks - 1
        token = part * (TILE // GROUP) + lax.broadcasted_iota(jnp.int32, (TILE, KB), 0) // GROUP
        key = lax.broadcasted_iota(jnp.int32, (TILE, KB), 1)
        visible = key <= (pos - last * PER_BLOCK) * SPAN + token
        keep(last, jnp.where(visible, score(last), -1e30))
        top[...] = jnp.broadcast_to(jnp.max(top[...], axis=1, keepdims=True), (TILE, HD))
        acc[...] = jnp.zeros_like(acc)

        def second_pass(b, carry):
            at = pl.multiple_of(b * KB, KB)
            rows = pl.ds(at, KB)
            peak = top[...]
            s = scores[b]
            s = jnp.concatenate([s[:, :HD] - peak, s[:, HD:] - peak], axis=1)
            weights = jnp.exp2(s * (SCALE * LOG2E))
            half_weights = weights.astype(BF16)
            scaled = weights * SCALE
            v = kv[rows, 5 * HD : 6 * HD]
            from_v = jnp.dot(
                half_weights,
                jnp.concatenate([kv[rows, 5 * HD : 10 * HD], ones], axis=1),
                preferred_element_type=F32,
            )
            v_ones = jnp.concatenate([v, ones], axis=1)
            q = rows_of(0)
            k = kv[rows, 0:HD]
            acc[:, 0:HD] += from_v[:, 0:HD]
            acc[:, HD : 2 * HD] += from_v[:, 5 * HD : 6 * HD]
            for t in range(P_SIZE):
                lhs = jnp.concatenate([rows_of(1 + t), q], axis=1)
                rhs = jnp.concatenate([k, kv[rows, (1 + t) * HD : (2 + t) * HD]], axis=1)
                weighted = (scaled * over_last(lhs, rhs)).astype(BF16)
                part_sum = jnp.dot(weighted, v_ones, preferred_element_type=F32)
                c = 2 * (1 + t) * HD
                acc[:, c : c + HD] += part_sum[:, :HD] + from_v[:, (1 + t) * HD : (2 + t) * HD]
                acc[:, c + HD : c + 2 * HD] += part_sum[:, HD:]
            return carry

        lax.fori_loop(0, blocks, second_pass, 0)
        inverse = 1.0 / acc[:, HD : 2 * HD]
        primal = acc[:, 0:HD] * inverse

        def put(k, value):
            out_ref[pl.ds(source, sources), k] = value.astype(BF16).reshape(sources, 256, HD)

        put(0, primal)
        for t in range(P_SIZE):
            c = 2 * (1 + t) * HD
            put(1 + t, (acc[:, c : c + HD] - primal * acc[:, c + HD : c + 2 * HD]) * inverse)
        return unused

    lax.fori_loop(0, 2 * HALF // TILE, tile, 0)


def attention(meta, x, kv, interpret=False):
    return pl.pallas_call(
        attend,
        out_shape=jax.ShapeDtypeStruct(x.shape, BF16),
        in_specs=[
            pl.BlockSpec(memory_space=pltpu.SMEM),
            pl.BlockSpec(memory_space=pltpu.VMEM),
            pl.BlockSpec(memory_space=pl.ANY),
        ],
        out_specs=pl.BlockSpec(memory_space=pltpu.VMEM),
        scratch_shapes=[
            pltpu.VMEM((SPANS * SPAN, WIDTH), BF16),
            pltpu.VMEM((BLOCKS, TILE, KB), F32),
            pltpu.VMEM((TILE, HD), F32),
            pltpu.VMEM((TILE, 10 * HD), F32),
            pltpu.SemaphoreType.DMA((SPANS,)),
        ],
        compiler_params=pltpu.CompilerParams(vmem_limit_bytes=40 * 2**20),
        interpret=interpret,
        name="attend",
    )(meta, x, kv)


def per_device(queries, query_tangents, keys, key_tangents, values, value_tangents, span_order):
    packed = jnp.concatenate(
        [
            keys.reshape(ROWS, KVH, HD),
            key_tangents.reshape(ROWS, KVH, P_SIZE * HD),
            values.reshape(ROWS, KVH, HD),
            value_tangents.reshape(ROWS, KVH, P_SIZE * HD),
        ],
        axis=2,
    )
    head_kv = lax.all_to_all(packed.transpose(1, 0, 2), "uly", 0, 0, tiled=True)
    kv = lax.all_gather(head_kv.reshape(ULY * ROWS, WIDTH), "blk", axis=0, tiled=True)

    q = queries.reshape(ROWS, ULY, GROUP, HD).transpose(1, 0, 2, 3).reshape(ULY, 1, 256, HD)
    qt = query_tangents.reshape(ROWS, ULY, GROUP, P_SIZE, HD).transpose(1, 3, 0, 2, 4)
    x = jnp.concatenate([q, qt.reshape(ULY, P_SIZE, 256, HD)], axis=1)
    x = lax.all_to_all(x, "uly", 0, 0, tiled=True)

    blk = lax.axis_index("blk").astype(jnp.int32)
    meta = jnp.concatenate([span_order, blk[None]])
    out = attention(meta, x, kv)
    out = lax.all_to_all(out, "uly", 0, 0, tiled=True).reshape(ULY, 1 + P_SIZE, ROWS, GROUP, HD)
    attention_out = out[:, 0].transpose(1, 0, 2, 3).reshape(ROWS, HQ, HD)
    tangent_out = out[:, 1:].transpose(2, 0, 3, 1, 4).reshape(ROWS, HQ, P_SIZE, HD)
    return attention_out, tangent_out


def solution(mesh):
    placed = (
        P(("blk", "uly"), None, None),
        P(("blk", "uly"), None, None, None),
        P(("blk", "uly"), None, None),
        P(("blk", "uly"), None, None, None),
        P(("blk", "uly"), None, None),
        P(("blk", "uly"), None, None, None),
        P(),
    )
    return jax.shard_map(
        per_device,
        mesh=mesh,
        in_specs=placed,
        out_specs=(P(("blk", "uly"), None, None), P(("blk", "uly"), None, None, None)),
        check_vma=False,
    )
```

```python
import math

import jax
import jax.numpy as jnp
from jax import lax
from jax.experimental import pallas as pl
from jax.experimental.pallas import tpu as pltpu
from jax.sharding import Mesh
from jax.sharding import PartitionSpec as P

HD = 128
HQ = 128
KVH = 8
P_SIZE = 4
GROUP = HQ // KVH
SPAN = 64
SPANS = 32
ULY = 8
ROWS = 16
KB = 256
PER_BLOCK = KB // SPAN
BLOCKS = SPANS // PER_BLOCK
PARTS = 2
HEADS = GROUP // PARTS
CHUNK = ROWS * HEADS
TILE = SPAN * HEADS
WIDTH = HD * (2 + 2 * P_SIZE)
SCALE = HD**-0.5
LOG2E = math.log2(math.e)
F32 = jnp.float32
BF16 = jnp.bfloat16
AXES = ("z", "xh", "core", "y", "xl")


def over_last(a, b):
    return lax.dot_general(a, b, (((1,), (1,)), ((), ())), preferred_element_type=F32)


def pieces_of(z, xh, core):
    found = []
    for other_core in range(2):
        at = 5 * other_core
        c = core ^ other_core
        for operand, step, halves in ((0, 0, (0, 1)), (1, 3, (0, 1)), (2, 1, (0, 1)), (3, 2, (0,)), (4, 2, (1,))):
            for place, h in enumerate(halves):
                block = (((z + step) % 4) * 2 + (xh ^ h)) * 2 + c
                for s in range(2):
                    found.append((at + operand, place * 2 * SPAN + s * SPAN, 2 * block + s))
    return found


def attend(meta, x_ref, *rest):
    pieces, (out_ref, kv, scores, top, acc, sems) = rest[:10], rest[10:]
    blk = meta[SPANS]
    first = 2 * blk

    for n, (operand, row, stored) in enumerate(pieces_of(blk // 4, (blk // 2) % 2, blk % 2)):
        at = pl.multiple_of(meta[stored] * SPAN, SPAN)
        pltpu.make_async_copy(
            pieces[operand].at[pl.ds(row, SPAN), :], kv.at[pl.ds(at, SPAN), :], sems.at[n]
        ).start()
    for n in range(SPANS):
        pltpu.make_async_copy(
            pieces[0].at[pl.ds(0, SPAN), :], kv.at[pl.ds(0, SPAN), :], sems.at[n]
        ).wait()

    ones = jnp.ones((KB, HD), BF16)

    def tile(half, unused):
        pos = meta[first + half]
        blocks = pos // PER_BLOCK + 1
        source = half * 4

        def rows_of(k):
            return x_ref[pl.ds(source, 4), k].reshape(TILE, HD)

        def score(b):
            at = pl.multiple_of(b * KB, KB)
            return over_last(rows_of(0), kv[pl.ds(at, KB), 0:HD])

        def keep(b, s):
            scores[b] = s
            top[...] = jnp.maximum(top[...], jnp.maximum(s[:, :HD], s[:, HD:]))

        top[...] = jnp.full((TILE, HD), -1e30, F32)

        def first_pass(b, carry):
            keep(b, score(b))
            return carry

        lax.fori_loop(0, blocks - 1, first_pass, 0)
        last = blocks - 1
        token = lax.broadcasted_iota(jnp.int32, (TILE, KB), 0) // HEADS
        key = lax.broadcasted_iota(jnp.int32, (TILE, KB), 1)
        visible = key <= (pos - last * PER_BLOCK) * SPAN + token
        keep(last, jnp.where(visible, score(last), -1e30))
        top[...] = jnp.broadcast_to(jnp.max(top[...], axis=1, keepdims=True), (TILE, HD))
        acc[...] = jnp.zeros_like(acc)

        def second_pass(b, carry):
            at = pl.multiple_of(b * KB, KB)
            rows = pl.ds(at, KB)
            peak = top[...]
            s = scores[b]
            s = jnp.concatenate([s[:, :HD] - peak, s[:, HD:] - peak], axis=1)
            weights = jnp.exp2(s * (SCALE * LOG2E))
            half_weights = weights.astype(BF16)
            scaled = weights * SCALE
            v = kv[rows, 5 * HD : 6 * HD]
            from_v = jnp.dot(
                half_weights,
                jnp.concatenate([kv[rows, 5 * HD : 10 * HD], ones], axis=1),
                preferred_element_type=F32,
            )
            v_ones = jnp.concatenate([v, ones], axis=1)
            q = rows_of(0)
            k = kv[rows, 0:HD]
            acc[:, 0:HD] += from_v[:, 0:HD]
            acc[:, HD : 2 * HD] += from_v[:, 5 * HD : 6 * HD]
            for t in range(P_SIZE):
                lhs = jnp.concatenate([rows_of(1 + t), q], axis=1)
                rhs = jnp.concatenate([k, kv[rows, (1 + t) * HD : (2 + t) * HD]], axis=1)
                weighted = (scaled * over_last(lhs, rhs)).astype(BF16)
                part_sum = jnp.dot(weighted, v_ones, preferred_element_type=F32)
                c = 2 * (1 + t) * HD
                acc[:, c : c + HD] += part_sum[:, :HD] + from_v[:, (1 + t) * HD : (2 + t) * HD]
                acc[:, c + HD : c + 2 * HD] += part_sum[:, HD:]
            return carry

        lax.fori_loop(0, blocks, second_pass, 0)
        inverse = 1.0 / acc[:, HD : 2 * HD]
        primal = acc[:, 0:HD] * inverse

        def put(k, value):
            out_ref[pl.ds(source, 4), k] = value.astype(BF16).reshape(4, CHUNK, HD)

        put(0, primal)
        for t in range(P_SIZE):
            c = 2 * (1 + t) * HD
            put(1 + t, (acc[:, c : c + HD] - primal * acc[:, c + HD : c + 2 * HD]) * inverse)
        return unused

    lax.fori_loop(0, 2, tile, 0)


def attention(meta, x, pieces):
    flops = 2 * 2 * TILE * 5 * KB * 11 * KB * HD
    return pl.pallas_call(
        attend,
        out_shape=jax.ShapeDtypeStruct(x.shape, BF16),
        in_specs=[
            pl.BlockSpec(memory_space=pltpu.SMEM),
            pl.BlockSpec(memory_space=pltpu.VMEM),
        ]
        + [pl.BlockSpec(memory_space=pl.ANY)] * len(pieces),
        out_specs=pl.BlockSpec(memory_space=pltpu.VMEM),
        scratch_shapes=[
            pltpu.VMEM((SPANS * SPAN, WIDTH), BF16),
            pltpu.VMEM((BLOCKS, TILE, KB), F32),
            pltpu.VMEM((TILE, HD), F32),
            pltpu.VMEM((TILE, 10 * HD), F32),
            pltpu.SemaphoreType.DMA((SPANS,)),
        ],
        compiler_params=pltpu.CompilerParams(vmem_limit_bytes=30 * 2**20),
        cost_estimate=pl.CostEstimate(flops=flops, transcendentals=0, bytes_accessed=8 * 2**20),
        name="attend",
    )(meta, x, *pieces)


def gather_blocks(own):
    beside = lax.ppermute(own, "xh", [(0, 1), (1, 0)])
    here = jnp.concatenate([own, beside], axis=0)
    up = [(i, (i + 1) % 4) for i in range(4)]
    down = [(i, (i + 3) % 4) for i in range(4)]
    below = lax.ppermute(here, "z", up)
    above = lax.ppermute(here, "z", down)
    far_low = lax.ppermute(below[: 2 * SPAN], "z", up)
    far_high = lax.ppermute(above[2 * SPAN :], "z", down)
    mine = [here, below, above, far_low, far_high]
    return mine + [lax.ppermute(a, "core", [(0, 1), (1, 0)]) for a in mine]


def per_device(queries, query_tangents, keys, key_tangents, values, value_tangents, span_order):
    packed = jnp.concatenate(
        [
            keys.reshape(ROWS, KVH, HD),
            key_tangents.reshape(ROWS, KVH, P_SIZE * HD),
            values.reshape(ROWS, KVH, HD),
            value_tangents.reshape(ROWS, KVH, P_SIZE * HD),
        ],
        axis=2,
    )
    heads = ("y", "xl")
    head_kv = lax.all_to_all(packed.transpose(1, 0, 2), heads, 0, 0, tiled=True)
    pieces = gather_blocks(head_kv.reshape(ULY * ROWS, WIDTH))

    q = queries.reshape(ROWS, ULY, PARTS, HEADS, HD).transpose(2, 1, 0, 3, 4)
    qt = query_tangents.reshape(ROWS, ULY, PARTS, HEADS, P_SIZE, HD).transpose(2, 1, 4, 0, 3, 5)
    blk = lax.axis_index(("z", "xh", "core")).astype(jnp.int32)
    meta = jnp.concatenate([span_order, blk[None]])
    got = []
    for part in range(PARTS):
        x = jnp.concatenate(
            [
                q[part].reshape(ULY, 1, CHUNK, HD),
                qt[part].reshape(ULY, P_SIZE, CHUNK, HD),
            ],
            axis=1,
        )
        got.append(lax.all_to_all(x, heads, 0, 0, tiled=True))
    sent = []
    for part in range(PARTS):
        out = attention(meta, got[part], pieces)
        out = lax.all_to_all(out, heads, 0, 0, tiled=True)
        sent.append(out.reshape(ULY, 1 + P_SIZE, ROWS, HEADS, HD))
    attention_out = jnp.stack([o[:, 0] for o in sent], axis=1)
    attention_out = attention_out.transpose(2, 0, 1, 3, 4).reshape(ROWS, HQ, HD)
    tangent_out = jnp.stack([o[:, 1:] for o in sent], axis=1)
    tangent_out = tangent_out.transpose(3, 0, 1, 4, 2, 5).reshape(ROWS, HQ, P_SIZE, HD)
    return attention_out, tangent_out


def solution(mesh):
    grid = Mesh(mesh.devices.reshape(4, 2, 2, 4, 2), AXES)
    rows = P(AXES)
    return jax.shard_map(
        per_device,
        mesh=grid,
        in_specs=(rows,) * 6 + (P(),),
        out_specs=(rows, rows),
        check_vma=False,
    )
```

```python
import functools
import math

import jax
import jax.numpy as jnp
from jax import lax
from jax.experimental import pallas as pl
from jax.experimental.pallas import tpu as pltpu
from jax.sharding import Mesh
from jax.sharding import PartitionSpec as P

HD = 128
HQ = 128
KVH = 8
P_SIZE = 4
GROUP = HQ // KVH
SPAN = 64
SPANS = 32
ULY = 8
ROWS = 16
KB = 256
PER_BLOCK = KB // SPAN
BLOCKS = SPANS // PER_BLOCK
PARTS = 2
TOKENS = ROWS // PARTS
CHUNK = TOKENS * GROUP
TILE = 4 * CHUNK
OUT = (ULY, TOKENS, 1 + P_SIZE, GROUP, HD)
WIDTH = HD * (2 + 2 * P_SIZE)
SCALE = HD**-0.5
LOG2E = math.log2(math.e)
F32 = jnp.float32
BF16 = jnp.bfloat16
AXES = ("z", "xh", "core", "y", "xl")


def over_last(a, b):
    return lax.dot_general(a, b, (((1,), (1,)), ((), ())), preferred_element_type=F32)


def pieces_of(z, xh, core):
    found = []
    for other_core in range(2):
        at = 5 * other_core
        c = core ^ other_core
        for operand, step, halves in ((0, 0, (0, 1)), (1, 3, (0, 1)), (2, 1, (0, 1)), (3, 2, (0,)), (4, 2, (1,))):
            for place, h in enumerate(halves):
                block = (((z + step) % 4) * 2 + (xh ^ h)) * 2 + c
                for s in range(2):
                    found.append((at + operand, place * 2 * SPAN + s * SPAN, 2 * block + s))
    return found


def attend(part, meta, x_ref, *rest):
    pieces, (out_ref, kv, scores, top, acc, woven, sems) = rest[:10], rest[10:]
    blk = meta[SPANS]
    first = 2 * blk

    for n, (operand, row, stored) in enumerate(pieces_of(blk // 4, (blk // 2) % 2, blk % 2)):
        at = pl.multiple_of(meta[stored] * SPAN, SPAN)
        pltpu.make_async_copy(
            pieces[operand].at[pl.ds(row, SPAN), :], kv.at[pl.ds(at, SPAN), :], sems.at[n]
        ).start()
    for n in range(SPANS):
        pltpu.make_async_copy(
            pieces[0].at[pl.ds(0, SPAN), :], kv.at[pl.ds(0, SPAN), :], sems.at[n]
        ).wait()

    ones = jnp.ones((KB, HD), BF16)

    def tile(half, unused):
        pos = meta[first + half]
        blocks = pos // PER_BLOCK + 1
        source = half * 4

        def rows_of(k):
            return x_ref[pl.ds(source, 4), k].reshape(TILE, HD)

        def score(b):
            at = pl.multiple_of(b * KB, KB)
            return over_last(rows_of(0), kv[pl.ds(at, KB), 0:HD])

        def keep(b, s):
            scores[b] = s
            top[...] = jnp.maximum(top[...], jnp.maximum(s[:, :HD], s[:, HD:]))

        top[...] = jnp.full((TILE, HD), -1e30, F32)

        def first_pass(b, carry):
            keep(b, score(b))
            return carry

        lax.fori_loop(0, blocks - 1, first_pass, 0)
        last = blocks - 1
        row = lax.broadcasted_iota(jnp.int32, (TILE, KB), 0)
        token = row // CHUNK * ROWS + part * TOKENS + row % CHUNK // GROUP
        key = lax.broadcasted_iota(jnp.int32, (TILE, KB), 1)
        visible = key <= (pos - last * PER_BLOCK) * SPAN + token
        keep(last, jnp.where(visible, score(last), -1e30))
        top[...] = jnp.broadcast_to(jnp.max(top[...], axis=1, keepdims=True), (TILE, HD))
        acc[...] = jnp.zeros_like(acc)

        def second_pass(b, carry):
            at = pl.multiple_of(b * KB, KB)
            rows = pl.ds(at, KB)
            peak = top[...]
            s = scores[b]
            s = jnp.concatenate([s[:, :HD] - peak, s[:, HD:] - peak], axis=1)
            weights = jnp.exp2(s * (SCALE * LOG2E))
            half_weights = weights.astype(BF16)
            scaled = weights * SCALE
            v = kv[rows, 5 * HD : 6 * HD]
            from_v = jnp.dot(
                half_weights,
                jnp.concatenate([kv[rows, 5 * HD : 10 * HD], ones], axis=1),
                preferred_element_type=F32,
            )
            v_ones = jnp.concatenate([v, ones], axis=1)
            q = rows_of(0)
            k = kv[rows, 0:HD]
            acc[:, 0:HD] += from_v[:, 0:HD]
            acc[:, HD : 2 * HD] += from_v[:, 5 * HD : 6 * HD]
            for t in range(P_SIZE):
                lhs = jnp.concatenate([rows_of(1 + t), q], axis=1)
                rhs = jnp.concatenate([k, kv[rows, (1 + t) * HD : (2 + t) * HD]], axis=1)
                weighted = (scaled * over_last(lhs, rhs)).astype(BF16)
                part_sum = jnp.dot(weighted, v_ones, preferred_element_type=F32)
                c = 2 * (1 + t) * HD
                acc[:, c : c + HD] += part_sum[:, :HD] + from_v[:, (1 + t) * HD : (2 + t) * HD]
                acc[:, c + HD : c + 2 * HD] += part_sum[:, HD:]
            return carry

        lax.fori_loop(0, blocks, second_pass, 0)
        inverse = 1.0 / acc[:, HD : 2 * HD]
        primal = acc[:, 0:HD] * inverse

        out_ref[pl.ds(source, 4), :, 0] = primal.astype(BF16).reshape(4, TOKENS, GROUP, HD)
        for t in range(P_SIZE):
            c = 2 * (1 + t) * HD
            value = (acc[:, c : c + HD] - primal * acc[:, c + HD : c + 2 * HD]) * inverse
            woven[pl.ds(t, TILE, stride=P_SIZE), :] = value
        for n in range(4):
            rows = woven[n * P_SIZE * CHUNK : (n + 1) * P_SIZE * CHUNK, :]
            out_ref[source + n, :, 1:] = rows.astype(BF16).reshape(TOKENS, P_SIZE, GROUP, HD)
        return unused

    lax.fori_loop(0, 2, tile, 0)


def attention(meta, x, pieces, part):
    flops = 2 * 2 * TILE * 5 * KB * 11 * KB * HD
    return pl.pallas_call(
        functools.partial(attend, part),
        grid=(1,),
        out_shape=jax.ShapeDtypeStruct(OUT, BF16),
        in_specs=[
            pl.BlockSpec(memory_space=pltpu.SMEM),
            pl.BlockSpec((ULY, 1 + P_SIZE, CHUNK, HD), lambda i: (0, 0, part, 0)),
        ]
        + [pl.BlockSpec(memory_space=pl.ANY)] * len(pieces),
        out_specs=pl.BlockSpec(OUT, lambda i: (0, 0, 0, 0, 0)),
        scratch_shapes=[
            pltpu.VMEM((SPANS * SPAN, WIDTH), BF16),
            pltpu.VMEM((BLOCKS, TILE, KB), F32),
            pltpu.VMEM((TILE, HD), F32),
            pltpu.VMEM((TILE, 10 * HD), F32),
            pltpu.VMEM((P_SIZE * TILE, HD), F32),
            pltpu.SemaphoreType.DMA((SPANS,)),
        ],
        compiler_params=pltpu.CompilerParams(vmem_limit_bytes=60 * 2**20),
        cost_estimate=pl.CostEstimate(flops=flops, transcendentals=0, bytes_accessed=8 * 2**20),
        name="attend",
    )(meta, x, *pieces)


def place(*refs):
    parts, (primal_ref, tangent_ref, sems) = refs[:PARTS], refs[PARTS:]
    copies = []
    for part in range(PARTS):
        rows = pl.ds(part * TOKENS, TOKENS)
        for g in range(ULY):
            copies.append((parts[part].at[g, :, 1:], tangent_ref.at[rows, g]))
            copies.append((parts[part].at[g, :, 0], primal_ref.at[rows, g]))
    copies = [pltpu.make_async_copy(a, b, sems.at[n]) for n, (a, b) in enumerate(copies)]
    for copy in copies:
        copy.start()
    for copy in copies:
        copy.wait()


def assemble(parts):
    return pl.pallas_call(
        place,
        out_shape=(
            jax.ShapeDtypeStruct((ROWS, ULY, GROUP, HD), BF16),
            jax.ShapeDtypeStruct((ROWS, ULY, P_SIZE, GROUP, HD), BF16),
        ),
        in_specs=[pl.BlockSpec(memory_space=pl.ANY)] * PARTS,
        out_specs=[pl.BlockSpec(memory_space=pl.ANY)] * 2,
        scratch_shapes=[pltpu.SemaphoreType.DMA((2 * PARTS * ULY,))],
        name="place",
    )(*parts)


def gather_blocks(own):
    beside = lax.ppermute(own, "xh", [(0, 1), (1, 0)])
    here = jnp.concatenate([own, beside], axis=0)
    up = [(i, (i + 1) % 4) for i in range(4)]
    down = [(i, (i + 3) % 4) for i in range(4)]
    below = lax.ppermute(here, "z", up)
    above = lax.ppermute(here, "z", down)
    far_low = lax.ppermute(below[: 2 * SPAN], "z", up)
    far_high = lax.ppermute(above[2 * SPAN :], "z", down)
    mine = [here, below, above, far_low, far_high]
    return mine + [lax.ppermute(a, "core", [(0, 1), (1, 0)]) for a in mine]


def per_device(queries, query_tangents, keys, key_tangents, values, value_tangents, span_order):
    packed = jnp.concatenate(
        [
            keys.reshape(ROWS, KVH, HD),
            key_tangents.reshape(ROWS, KVH, P_SIZE * HD),
            values.reshape(ROWS, KVH, HD),
            value_tangents.reshape(ROWS, KVH, P_SIZE * HD),
        ],
        axis=2,
    )
    heads = ("y", "xl")
    head_kv = lax.all_to_all(packed.transpose(1, 0, 2), heads, 0, 0, tiled=True)
    pieces = gather_blocks(head_kv.reshape(ULY * ROWS, WIDTH))

    q = queries.reshape(ROWS, ULY, GROUP, HD).transpose(1, 0, 2, 3)
    qt = query_tangents.reshape(ROWS, ULY, GROUP, P_SIZE, HD).transpose(1, 3, 0, 2, 4)
    blk = lax.axis_index(("z", "xh", "core")).astype(jnp.int32)
    meta = jnp.concatenate([span_order, blk[None]])
    x = jnp.concatenate(
        [
            q.reshape(ULY, 1, ROWS * GROUP, HD),
            qt.reshape(ULY, P_SIZE, ROWS * GROUP, HD),
        ],
        axis=1,
    )
    x = lax.all_to_all(x, heads, 0, 0, tiled=True)
    sent = []
    for part in range(PARTS):
        out = attention(meta, x, pieces, part)
        sent.append(lax.all_to_all(out, heads, 0, 0, tiled=True))
    primal, tangent = assemble(sent)
    return primal.reshape(ROWS, HQ, HD), tangent.reshape(ROWS, HQ, P_SIZE, HD)


def solution(mesh):
    grid = Mesh(mesh.devices.reshape(4, 2, 2, 4, 2), AXES)
    rows = P(AXES)
    return jax.shard_map(
        per_device,
        mesh=grid,
        in_specs=(rows,) * 6 + (P(),),
        out_specs=(rows, rows),
        check_vma=False,
    )
```

```python
import functools
import math

import jax
import jax.numpy as jnp
from jax import lax
from jax.experimental import pallas as pl
from jax.experimental.pallas import tpu as pltpu
from jax.sharding import Mesh
from jax.sharding import PartitionSpec as P

HD = 128
HQ = 128
KVH = 8
P_SIZE = 4
GROUP = HQ // KVH
SPAN = 64
SPANS = 32
ULY = 8
ROWS = 16
KB = 256
PER_BLOCK = KB // SPAN
BLOCKS = SPANS // PER_BLOCK
PARTS = 2
TOKENS = ROWS // PARTS
CHUNK = TOKENS * GROUP
TILE = 4 * CHUNK
OUT = (ULY, TOKENS, 1 + P_SIZE, GROUP, HD)
WIDTH = HD * (2 + 2 * P_SIZE)
SCALE = HD**-0.5
LOG2E = math.log2(math.e)
F32 = jnp.float32
BF16 = jnp.bfloat16
AXES = ("z", "xh", "core", "y", "xl")


def over_last(a, b):
    return lax.dot_general(a, b, (((1,), (1,)), ((), ())), preferred_element_type=F32)


def pieces_of(z, core):
    found = []
    for other_core in range(2):
        at = 5 * other_core
        c = core ^ other_core
        for operand, step, halves in ((0, 0, (0, 1)), (1, 3, (0, 1)), (2, 1, (0, 1)), (3, 2, (0,)), (4, 2, (1,))):
            for place, h in enumerate(halves):
                block = (((z + step) % 4) * 2 + h) * 2 + c
                for s in range(2):
                    found.append((at + operand, place * 2 * SPAN + s * SPAN, 2 * block + s))
    return found


def attend(part, meta, x_ref, *rest):
    pieces, (out_ref, kv, scores, top, acc, woven, sems) = rest[:10], rest[10:]
    blk = meta[SPANS]
    first = 2 * blk

    for n, (operand, row, stored) in enumerate(pieces_of(blk // 4, blk % 2)):
        at = pl.multiple_of(meta[stored] * SPAN, SPAN)
        pltpu.make_async_copy(
            pieces[operand].at[pl.ds(row, SPAN), :], kv.at[pl.ds(at, SPAN), :], sems.at[n]
        ).start()
    for n in range(SPANS):
        pltpu.make_async_copy(
            pieces[0].at[pl.ds(0, SPAN), :], kv.at[pl.ds(0, SPAN), :], sems.at[n]
        ).wait()

    ones = jnp.ones((KB, HD), BF16)

    def tile(half, unused):
        pos = meta[first + half]
        blocks = pos // PER_BLOCK + 1
        source = half * 4

        def rows_of(k):
            return x_ref[pl.ds(source, 4), k].reshape(TILE, HD)

        def score(b):
            at = pl.multiple_of(b * KB, KB)
            return over_last(rows_of(0), kv[pl.ds(at, KB), 0:HD])

        def keep(b, s):
            scores[b] = s
            top[...] = jnp.maximum(top[...], jnp.maximum(s[:, :HD], s[:, HD:]))

        top[...] = jnp.full((TILE, HD), -1e30, F32)

        def first_pass(b, carry):
            keep(b, score(b))
            return carry

        lax.fori_loop(0, blocks - 1, first_pass, 0)
        last = blocks - 1
        row = lax.broadcasted_iota(jnp.int32, (TILE, KB), 0)
        token = row // CHUNK * ROWS + part * TOKENS + row % CHUNK // GROUP
        key = lax.broadcasted_iota(jnp.int32, (TILE, KB), 1)
        visible = key <= (pos - last * PER_BLOCK) * SPAN + token
        keep(last, jnp.where(visible, score(last), -1e30))
        top[...] = jnp.broadcast_to(jnp.max(top[...], axis=1, keepdims=True), (TILE, HD))
        acc[...] = jnp.zeros_like(acc)

        def second_pass(b, carry):
            at = pl.multiple_of(b * KB, KB)
            rows = pl.ds(at, KB)
            peak = top[...]
            s = scores[b]
            s = jnp.concatenate([s[:, :HD] - peak, s[:, HD:] - peak], axis=1)
            weights = jnp.exp2(s * (SCALE * LOG2E))
            half_weights = weights.astype(BF16)
            scaled = weights * SCALE
            v = kv[rows, 5 * HD : 6 * HD]
            from_v = jnp.dot(
                half_weights,
                jnp.concatenate([kv[rows, 5 * HD : 10 * HD], ones], axis=1),
                preferred_element_type=F32,
            )
            v_ones = jnp.concatenate([v, ones], axis=1)
            q = rows_of(0)
            k = kv[rows, 0:HD]
            acc[:, 0:HD] += from_v[:, 0:HD]
            acc[:, HD : 2 * HD] += from_v[:, 5 * HD : 6 * HD]
            for t in range(P_SIZE):
                lhs = jnp.concatenate([rows_of(1 + t), q], axis=1)
                rhs = jnp.concatenate([k, kv[rows, (1 + t) * HD : (2 + t) * HD]], axis=1)
                weighted = (scaled * over_last(lhs, rhs)).astype(BF16)
                part_sum = jnp.dot(weighted, v_ones, preferred_element_type=F32)
                c = 2 * (1 + t) * HD
                acc[:, c : c + HD] += part_sum[:, :HD] + from_v[:, (1 + t) * HD : (2 + t) * HD]
                acc[:, c + HD : c + 2 * HD] += part_sum[:, HD:]
            return carry

        lax.fori_loop(0, blocks, second_pass, 0)
        inverse = 1.0 / acc[:, HD : 2 * HD]
        primal = acc[:, 0:HD] * inverse

        out_ref[pl.ds(source, 4), :, 0] = primal.astype(BF16).reshape(4, TOKENS, GROUP, HD)
        for t in range(P_SIZE):
            c = 2 * (1 + t) * HD
            value = (acc[:, c : c + HD] - primal * acc[:, c + HD : c + 2 * HD]) * inverse
            woven[pl.ds(t, TILE, stride=P_SIZE), :] = value
        for n in range(4):
            rows = woven[n * P_SIZE * CHUNK : (n + 1) * P_SIZE * CHUNK, :]
            out_ref[source + n, :, 1:] = rows.astype(BF16).reshape(TOKENS, P_SIZE, GROUP, HD)
        return unused

    lax.fori_loop(0, 2, tile, 0)


def attention(meta, x, pieces, part):
    flops = 2 * 2 * TILE * 5 * KB * 11 * KB * HD
    return pl.pallas_call(
        functools.partial(attend, part),
        grid=(1,),
        out_shape=jax.ShapeDtypeStruct(OUT, BF16),
        in_specs=[
            pl.BlockSpec(memory_space=pltpu.SMEM),
            pl.BlockSpec((ULY, 1 + P_SIZE, CHUNK, HD), lambda i: (0, 0, part, 0)),
        ]
        + [pl.BlockSpec(memory_space=pl.ANY)] * len(pieces),
        out_specs=pl.BlockSpec(OUT, lambda i: (0, 0, 0, 0, 0)),
        scratch_shapes=[
            pltpu.VMEM((SPANS * SPAN, WIDTH), BF16),
            pltpu.VMEM((BLOCKS, TILE, KB), F32),
            pltpu.VMEM((TILE, HD), F32),
            pltpu.VMEM((TILE, 10 * HD), F32),
            pltpu.VMEM((P_SIZE * TILE, HD), F32),
            pltpu.SemaphoreType.DMA((SPANS,)),
        ],
        compiler_params=pltpu.CompilerParams(vmem_limit_bytes=60 * 2**20),
        cost_estimate=pl.CostEstimate(flops=flops, transcendentals=0, bytes_accessed=8 * 2**20),
        name="attend",
    )(meta, x, *pieces)


def place(part_ref, *refs):
    primal_ref, tangent_ref = refs[-2:]
    for g in range(ULY):
        primal_ref[:, g] = part_ref[g, :, 0]
        tangent_ref[:, g] = part_ref[g, :, 1:]


def assemble(parts):
    step = 2
    steps = TOKENS // step
    placed = ()
    for n, part in enumerate(parts):
        placed = pl.pallas_call(
            place,
            grid=(steps,),
            out_shape=(
                jax.ShapeDtypeStruct((ROWS, ULY, GROUP, HD), BF16),
                jax.ShapeDtypeStruct((ROWS, ULY, P_SIZE, GROUP, HD), BF16),
            ),
            in_specs=[pl.BlockSpec((ULY, step, 1 + P_SIZE, GROUP, HD), lambda i: (0, i, 0, 0, 0))]
            + [pl.BlockSpec(memory_space=pl.ANY)] * len(placed),
            out_specs=(
                pl.BlockSpec((step, ULY, GROUP, HD), lambda i, n=n: (n * steps + i, 0, 0, 0)),
                pl.BlockSpec(
                    (step, ULY, P_SIZE, GROUP, HD), lambda i, n=n: (n * steps + i, 0, 0, 0, 0)
                ),
            ),
            input_output_aliases={1 + k: k for k in range(len(placed))},
            name="place",
        )(part, *placed)
    return placed


def gather_blocks(here):
    up = [(i, (i + 1) % 4) for i in range(4)]
    down = [(i, (i + 3) % 4) for i in range(4)]
    below = lax.ppermute(here, "z", up)
    above = lax.ppermute(here, "z", down)
    far_low = lax.ppermute(below[: 2 * SPAN], "z", up)
    far_high = lax.ppermute(above[2 * SPAN :], "z", down)
    mine = [here, below, above, far_low, far_high]
    return mine + [lax.ppermute(a, "core", [(0, 1), (1, 0)]) for a in mine]


def per_device(queries, query_tangents, keys, key_tangents, values, value_tangents, span_order):
    packed = jnp.concatenate(
        [
            keys.reshape(ROWS, KVH, HD),
            key_tangents.reshape(ROWS, KVH, P_SIZE * HD),
            values.reshape(ROWS, KVH, HD),
            value_tangents.reshape(ROWS, KVH, P_SIZE * HD),
        ],
        axis=2,
    )
    heads = ("y", "xl")
    packed = packed.transpose(1, 0, 2)
    packed = jnp.concatenate([packed, packed], axis=0)
    head_kv = lax.all_to_all(packed, ("xh",) + heads, 0, 0, tiled=True)
    pieces = gather_blocks(head_kv.reshape(2 * ULY * ROWS, WIDTH))

    q = queries.reshape(ROWS, ULY, GROUP, HD).transpose(1, 0, 2, 3)
    qt = query_tangents.reshape(ROWS, ULY, GROUP, P_SIZE, HD).transpose(1, 3, 0, 2, 4)
    blk = lax.axis_index(("z", "xh", "core")).astype(jnp.int32)
    meta = jnp.concatenate([span_order, blk[None]])
    x = jnp.concatenate(
        [
            q.reshape(ULY, 1, ROWS * GROUP, HD),
            qt.reshape(ULY, P_SIZE, ROWS * GROUP, HD),
        ],
        axis=1,
    )
    x = lax.all_to_all(x, heads, 0, 0, tiled=True)
    sent = []
    for part in range(PARTS):
        out = attention(meta, x, pieces, part)
        sent.append(lax.all_to_all(out, heads, 0, 0, tiled=True))
    primal, tangent = assemble(sent)
    return primal.reshape(ROWS, HQ, HD), tangent.reshape(ROWS, HQ, P_SIZE, HD)


def solution(mesh):
    grid = Mesh(mesh.devices.reshape(4, 2, 2, 4, 2), AXES)
    rows = P(AXES)
    return jax.shard_map(
        per_device,
        mesh=grid,
        in_specs=(rows,) * 6 + (P(),),
        out_specs=(rows, rows),
        check_vma=False,
    )
```

```python
import functools
import math

import jax
import jax.numpy as jnp
from jax import lax
from jax.experimental import pallas as pl
from jax.experimental.pallas import tpu as pltpu
from jax.sharding import Mesh
from jax.sharding import PartitionSpec as P

HD = 128
HQ = 128
KVH = 8
P_SIZE = 4
GROUP = HQ // KVH
SPAN = 64
SPANS = 32
ULY = 8
ROWS = 16
KB = 256
PER_BLOCK = KB // SPAN
BLOCKS = SPANS // PER_BLOCK
PARTS = 2
TOKENS = ROWS // PARTS
CHUNK = TOKENS * GROUP
TILE = 4 * CHUNK
OUT = (ULY, TOKENS, 1 + P_SIZE, GROUP, HD)
WIDTH = HD * (2 + 2 * P_SIZE)
SCALE = HD**-0.5
LIMIT = 34
LOG2E = math.log2(math.e)
F32 = jnp.float32
BF16 = jnp.bfloat16
AXES = ("z", "xh", "core", "y", "xl")


def over_last(a, b):
    return lax.dot_general(a, b, (((1,), (1,)), ((), ())), preferred_element_type=F32)


def pieces_of(z, core):
    found = []
    for other_core in range(2):
        at = 5 * other_core
        c = core ^ other_core
        for operand, step, halves in ((0, 0, (0, 1)), (1, 3, (0, 1)), (2, 1, (0, 1)), (3, 2, (0,)), (4, 2, (1,))):
            for place, h in enumerate(halves):
                block = (((z + step) % 4) * 2 + h) * 2 + c
                for s in range(2):
                    found.append((at + operand, place * 2 * SPAN + s * SPAN, 2 * block + s))
    return found


def attend(part, meta, x_ref, *rest):
    pieces, (out_hbm, kv, scores, top, acc, woven, out_ref, sems, out_sems) = rest[:10], rest[10:]
    blk = meta[SPANS]
    first = 2 * blk

    def fetch(columns, sem, operand=0, row=0, at=0):
        rows = pl.ds(at, SPAN)
        return pltpu.make_async_copy(
            pieces[operand].at[pl.ds(row, SPAN), columns], kv.at[rows, columns], sem
        )

    only_keys, others = slice(0, HD), slice(HD, WIDTH)
    spans = pieces_of(blk // 4, blk % 2)
    for columns, group in ((only_keys, 0), (others, 1)):
        for n, (operand, row, stored) in enumerate(spans):
            at = pl.multiple_of(meta[stored] * SPAN, SPAN)
            fetch(columns, sems.at[group, n], operand, row, at).start()
    for n in range(SPANS):
        fetch(only_keys, sems.at[0, n]).wait()

    ones = jnp.ones((KB, HD), BF16)

    def tile(half, unused):
        pos = meta[first + half]
        blocks = pos // PER_BLOCK + 1
        source = half * 4

        def rows_of(k):
            rows = slice(part * CHUNK, (part + 1) * CHUNK)
            return x_ref[pl.ds(source, 4), k, rows].reshape(TILE, HD)

        def score(b):
            at = pl.multiple_of(b * KB, KB)
            return over_last(rows_of(0), kv[pl.ds(at, KB), 0:HD])

        def keep(b, s):
            scores[b] = s
            top[...] = jnp.maximum(top[...], jnp.maximum(s[:, :HD], s[:, HD:]))

        top[...] = jnp.full((TILE, HD), -1e30, F32)

        def first_pass(b, carry):
            keep(b, score(b))
            return carry

        lax.fori_loop(0, blocks - 1, first_pass, 0)
        last = blocks - 1
        row = lax.broadcasted_iota(jnp.int32, (TILE, KB), 0)
        token = row // CHUNK * ROWS + part * TOKENS + row % CHUNK // GROUP
        key = lax.broadcasted_iota(jnp.int32, (TILE, KB), 1)
        visible = key <= (pos - last * PER_BLOCK) * SPAN + token
        keep(last, jnp.where(visible, score(last), -1e30))
        top[...] = jnp.broadcast_to(jnp.max(top[...], axis=1, keepdims=True), (TILE, HD))
        acc[...] = jnp.zeros_like(acc)

        @pl.when(half == 0)
        def _():
            for n in range(SPANS):
                fetch(others, sems.at[1, n]).wait()

        def second_pass(b, carry):
            at = pl.multiple_of(b * KB, KB)
            rows = pl.ds(at, KB)
            peak = top[...]
            s = scores[b]
            s = jnp.concatenate([s[:, :HD] - peak, s[:, HD:] - peak], axis=1)
            weights = jnp.exp2(s * (SCALE * LOG2E))
            half_weights = weights.astype(BF16)
            scaled = weights * SCALE
            v = kv[rows, 5 * HD : 6 * HD]
            from_v = jnp.dot(
                half_weights,
                jnp.concatenate([kv[rows, 5 * HD : 10 * HD], ones], axis=1),
                preferred_element_type=F32,
            )
            v_ones = jnp.concatenate([v, ones], axis=1)
            q = rows_of(0)
            k = kv[rows, 0:HD]
            acc[:, 0:HD] += from_v[:, 0:HD]
            acc[:, HD : 2 * HD] += from_v[:, 5 * HD : 6 * HD]
            for t in range(P_SIZE):
                lhs = jnp.concatenate([rows_of(1 + t), q], axis=1)
                rhs = jnp.concatenate([k, kv[rows, (1 + t) * HD : (2 + t) * HD]], axis=1)
                weighted = (scaled * over_last(lhs, rhs)).astype(BF16)
                part_sum = jnp.dot(weighted, v_ones, preferred_element_type=F32)
                c = 2 * (1 + t) * HD
                acc[:, c : c + HD] += part_sum[:, :HD] + from_v[:, (1 + t) * HD : (2 + t) * HD]
                acc[:, c + HD : c + 2 * HD] += part_sum[:, HD:]
            return carry

        lax.fori_loop(0, blocks, second_pass, 0)
        inverse = 1.0 / acc[:, HD : 2 * HD]
        primal = acc[:, 0:HD] * inverse

        out_ref[pl.ds(source, 4), :, 0] = primal.astype(BF16).reshape(4, TOKENS, GROUP, HD)
        for t in range(P_SIZE):
            c = 2 * (1 + t) * HD
            value = (acc[:, c : c + HD] - primal * acc[:, c + HD : c + 2 * HD]) * inverse
            woven[pl.ds(t, TILE, stride=P_SIZE), :] = value
        for n in range(4):
            rows = woven[n * P_SIZE * CHUNK : (n + 1) * P_SIZE * CHUNK, :]
            out_ref[source + n, :, 1:] = rows.astype(BF16).reshape(TOKENS, P_SIZE, GROUP, HD)
        send(half).start()
        return unused

    def send(half):
        rows = pl.ds(half * 4, 4)
        return pltpu.make_async_copy(out_ref.at[rows], out_hbm.at[rows], out_sems.at[half])

    lax.fori_loop(0, 2, tile, 0)
    for half in range(2):
        send(half).wait()


def attention(meta, x, pieces, part):
    flops = 2 * 2 * TILE * 5 * KB * 11 * KB * HD
    return pl.pallas_call(
        functools.partial(attend, part),
        out_shape=pltpu.HBM(OUT, BF16),
        in_specs=[
            pl.BlockSpec(memory_space=pltpu.SMEM),
            pl.BlockSpec(memory_space=pltpu.VMEM),
        ]
        + [pl.BlockSpec(memory_space=pltpu.HBM)] * len(pieces),
        out_specs=pl.BlockSpec(memory_space=pltpu.HBM),
        scratch_shapes=[
            pltpu.VMEM((SPANS * SPAN, WIDTH), BF16),
            pltpu.VMEM((BLOCKS, TILE, KB), F32),
            pltpu.VMEM((TILE, HD), F32),
            pltpu.VMEM((TILE, 10 * HD), F32),
            pltpu.VMEM((P_SIZE * TILE, HD), F32),
            pltpu.VMEM(OUT, BF16),
            pltpu.SemaphoreType.DMA((2, SPANS)),
            pltpu.SemaphoreType.DMA((2,)),
        ],
        compiler_params=pltpu.CompilerParams(vmem_limit_bytes=LIMIT * 2**20),
        cost_estimate=pl.CostEstimate(flops=flops, transcendentals=0, bytes_accessed=8 * 2**20),
        name="attend",
    )(meta, x, *pieces)


def place(part, part_ref, *refs):
    primal_ref, tangent_ref, sems = refs[-3:]
    rows = pl.ds(part * TOKENS, TOKENS)
    copies = []
    for g in range(ULY):
        copies.append((part_ref.at[g, :, 1:], tangent_ref.at[rows, g]))
        copies.append((part_ref.at[g, :, 0], primal_ref.at[rows, g]))
    copies = [pltpu.make_async_copy(a, b, sems.at[n]) for n, (a, b) in enumerate(copies)]
    for copy in copies:
        copy.start()
    for copy in copies:
        copy.wait()


def assemble(parts):
    placed = ()
    for n, part in enumerate(parts):
        placed = pl.pallas_call(
            functools.partial(place, n),
            out_shape=(
                jax.ShapeDtypeStruct((ROWS, ULY, GROUP, HD), BF16),
                jax.ShapeDtypeStruct((ROWS, ULY, P_SIZE, GROUP, HD), BF16),
            ),
            in_specs=[pl.BlockSpec(memory_space=pltpu.VMEM)]
            + [pl.BlockSpec(memory_space=pltpu.HBM)] * len(placed),
            out_specs=(pl.BlockSpec(memory_space=pltpu.HBM),) * 2,
            scratch_shapes=[pltpu.SemaphoreType.DMA((2 * ULY,))],
            input_output_aliases={1 + k: k for k in range(len(placed))},
            compiler_params=pltpu.CompilerParams(vmem_limit_bytes=8 * 2**20),
            name="place",
        )(part, *placed)
    return placed


def gather_blocks(here):
    up = [(i, (i + 1) % 4) for i in range(4)]
    down = [(i, (i + 3) % 4) for i in range(4)]
    below = lax.ppermute(here, "z", up)
    above = lax.ppermute(here, "z", down)
    far_low = lax.ppermute(below[: 2 * SPAN], "z", up)
    far_high = lax.ppermute(above[2 * SPAN :], "z", down)
    mine = [here, below, above, far_low, far_high]
    return mine + [lax.ppermute(a, "core", [(0, 1), (1, 0)]) for a in mine]


def per_device(queries, query_tangents, keys, key_tangents, values, value_tangents, span_order):
    packed = jnp.concatenate(
        [
            keys.reshape(ROWS, KVH, HD),
            key_tangents.reshape(ROWS, KVH, P_SIZE * HD),
            values.reshape(ROWS, KVH, HD),
            value_tangents.reshape(ROWS, KVH, P_SIZE * HD),
        ],
        axis=2,
    )
    heads = ("y", "xl")
    packed = packed.transpose(1, 0, 2)
    packed = jnp.concatenate([packed, packed], axis=0)
    head_kv = lax.all_to_all(packed, ("xh",) + heads, 0, 0, tiled=True)
    pieces = gather_blocks(head_kv.reshape(2 * ULY * ROWS, WIDTH))

    q = queries.reshape(ROWS, ULY, GROUP, HD).transpose(1, 0, 2, 3)
    qt = query_tangents.reshape(ROWS, ULY, GROUP, P_SIZE, HD).transpose(1, 3, 0, 2, 4)
    blk = lax.axis_index(("z", "xh", "core")).astype(jnp.int32)
    meta = jnp.concatenate([span_order, blk[None]])
    x = jnp.concatenate(
        [
            q.reshape(ULY, 1, ROWS * GROUP, HD),
            qt.reshape(ULY, P_SIZE, ROWS * GROUP, HD),
        ],
        axis=1,
    )
    x = lax.all_to_all(x, heads, 0, 0, tiled=True)
    sent = []
    for part in range(PARTS):
        out = attention(meta, x, pieces, part)
        sent.append(lax.all_to_all(out, heads, 0, 0, tiled=True))
    primal, tangent = assemble(sent)
    return primal.reshape(ROWS, HQ, HD), tangent.reshape(ROWS, HQ, P_SIZE, HD)


def solution(mesh):
    grid = Mesh(mesh.devices.reshape(4, 2, 2, 4, 2), AXES)
    rows = P(AXES)
    return jax.shard_map(
        per_device,
        mesh=grid,
        in_specs=(rows,) * 6 + (P(),),
        out_specs=(rows, rows),
        check_vma=False,
    )
```

```python
import functools
import math

import jax
import jax.numpy as jnp
from jax import lax
from jax.experimental import pallas as pl
from jax.experimental.pallas import tpu as pltpu
from jax.sharding import Mesh
from jax.sharding import PartitionSpec as P

HD = 128
HQ = 128
KVH = 8
P_SIZE = 4
GROUP = HQ // KVH
SPAN = 64
SPANS = 32
ULY = 8
ROWS = 16
KB = 256
PER_BLOCK = KB // SPAN
BLOCKS = SPANS // PER_BLOCK
PARTS = 2
TOKENS = ROWS // PARTS
CHUNK = TOKENS * GROUP
TILE = 4 * CHUNK
OUT = (ULY, TOKENS, 1 + P_SIZE, GROUP, HD)
WIDTH = HD * (2 + 2 * P_SIZE)
SCALE = HD**-0.5
LIMIT = 34
LOG2E = math.log2(math.e)
F32 = jnp.float32
BF16 = jnp.bfloat16
AXES = ("z", "xh", "core", "y", "xl")


def over_last(a, b):
    return lax.dot_general(a, b, (((1,), (1,)), ((), ())), preferred_element_type=F32)


def pieces_of(z, core):
    found = []
    for other_core in range(2):
        at = 5 * other_core
        c = core ^ other_core
        for operand, step, halves in ((0, 0, (0, 1)), (1, 3, (0, 1)), (2, 1, (0, 1)), (3, 2, (0,)), (4, 2, (1,))):
            for place, h in enumerate(halves):
                block = (((z + step) % 4) * 2 + h) * 2 + c
                for s in range(2):
                    found.append((at + operand, place * 2 * SPAN + s * SPAN, 2 * block + s))
    return found


def attend(part, meta, x_ref, *rest):
    pieces, (out_hbm, kv, scores, top, acc, woven, out_ref, sems, out_sems) = rest[:10], rest[10:]
    blk = meta[SPANS]
    first = 2 * blk

    def fetch(columns, sem, operand=0, row=0, at=0):
        rows = pl.ds(at, SPAN)
        return pltpu.make_async_copy(
            pieces[operand].at[pl.ds(row, SPAN), columns], kv.at[rows, columns], sem
        )

    only_keys, others = slice(0, HD), slice(HD, WIDTH)
    spans = pieces_of(blk // 4, blk % 2)
    for columns, group in ((only_keys, 0), (others, 1)):
        for n, (operand, row, stored) in enumerate(spans):
            at = pl.multiple_of(meta[stored] * SPAN, SPAN)
            fetch(columns, sems.at[group, n], operand, row, at).start()
    for n in range(SPANS):
        fetch(only_keys, sems.at[0, n]).wait()

    ones = jnp.ones((KB, HD), BF16)

    def tile(half, unused):
        pos = meta[first + half]
        blocks = pos // PER_BLOCK + 1
        source = half * 4

        def rows_of(k):
            rows = slice(part * CHUNK, (part + 1) * CHUNK)
            return x_ref[pl.ds(source, 4), k, rows].reshape(TILE, HD)

        def score(b):
            at = pl.multiple_of(b * KB, KB)
            return over_last(rows_of(0), kv[pl.ds(at, KB), 0:HD])

        def keep(b, s):
            scores[b] = s
            top[...] = jnp.maximum(top[...], jnp.maximum(s[:, :HD], s[:, HD:]))

        top[...] = jnp.full((TILE, HD), -1e30, F32)

        def first_pass(b, carry):
            keep(b, score(b))
            return carry

        lax.fori_loop(0, blocks - 1, first_pass, 0)
        last = blocks - 1
        row = lax.broadcasted_iota(jnp.int32, (TILE, KB), 0)
        token = row // CHUNK * ROWS + part * TOKENS + row % CHUNK // GROUP
        key = lax.broadcasted_iota(jnp.int32, (TILE, KB), 1)
        visible = key <= (pos - last * PER_BLOCK) * SPAN + token
        keep(last, jnp.where(visible, score(last), -1e30))
        top[...] = jnp.broadcast_to(jnp.max(top[...], axis=1, keepdims=True), (TILE, HD))
        acc[...] = jnp.zeros_like(acc)

        @pl.when(half == 0)
        def _():
            for n in range(SPANS):
                fetch(others, sems.at[1, n]).wait()

        def second_pass(b, carry):
            at = pl.multiple_of(b * KB, KB)
            rows = pl.ds(at, KB)
            peak = top[...]
            s = scores[b]
            s = jnp.concatenate([s[:, :HD] - peak, s[:, HD:] - peak], axis=1)
            weights = jnp.exp2(s * (SCALE * LOG2E))
            half_weights = weights.astype(BF16)
            scaled = weights * SCALE
            v = kv[rows, 5 * HD : 6 * HD]
            from_v = jnp.dot(
                half_weights,
                jnp.concatenate([kv[rows, 5 * HD : 10 * HD], ones], axis=1),
                preferred_element_type=F32,
            )
            v_ones = jnp.concatenate([v, ones], axis=1)
            q = rows_of(0)
            k = kv[rows, 0:HD]
            acc[:, 0:HD] += from_v[:, 0:HD]
            acc[:, HD : 2 * HD] += from_v[:, 5 * HD : 6 * HD]
            for t in range(P_SIZE):
                lhs = jnp.concatenate([rows_of(1 + t), q], axis=1)
                rhs = jnp.concatenate([k, kv[rows, (1 + t) * HD : (2 + t) * HD]], axis=1)
                weighted = (scaled * over_last(lhs, rhs)).astype(BF16)
                part_sum = jnp.dot(weighted, v_ones, preferred_element_type=F32)
                c = 2 * (1 + t) * HD
                acc[:, c : c + HD] += part_sum[:, :HD] + from_v[:, (1 + t) * HD : (2 + t) * HD]
                acc[:, c + HD : c + 2 * HD] += part_sum[:, HD:]
            return carry

        lax.fori_loop(0, blocks, second_pass, 0)
        inverse = 1.0 / acc[:, HD : 2 * HD]
        primal = acc[:, 0:HD] * inverse

        out_ref[pl.ds(source, 4), :, 0] = primal.astype(BF16).reshape(4, TOKENS, GROUP, HD)
        for t in range(P_SIZE):
            c = 2 * (1 + t) * HD
            value = (acc[:, c : c + HD] - primal * acc[:, c + HD : c + 2 * HD]) * inverse
            woven[pl.ds(t, TILE, stride=P_SIZE), :] = value
        for n in range(4):
            rows = woven[n * P_SIZE * CHUNK : (n + 1) * P_SIZE * CHUNK, :]
            out_ref[source + n, :, 1:] = rows.astype(BF16).reshape(TOKENS, P_SIZE, GROUP, HD)
        send(half).start()
        return unused

    def send(half):
        rows = pl.ds(half * 4, 4)
        return pltpu.make_async_copy(out_ref.at[rows], out_hbm.at[rows], out_sems.at[half])

    lax.fori_loop(0, 2, tile, 0)
    for half in range(2):
        send(half).wait()


def attention(meta, x, pieces, part):
    flops = 2 * 2 * TILE * 5 * KB * 11 * KB * HD
    return pl.pallas_call(
        functools.partial(attend, part),
        out_shape=pltpu.HBM(OUT, BF16),
        in_specs=[
            pl.BlockSpec(memory_space=pltpu.SMEM),
            pl.BlockSpec(memory_space=pltpu.VMEM),
        ]
        + [pl.BlockSpec(memory_space=pltpu.HBM)] * len(pieces),
        out_specs=pl.BlockSpec(memory_space=pltpu.HBM),
        scratch_shapes=[
            pltpu.VMEM((SPANS * SPAN, WIDTH), BF16),
            pltpu.VMEM((BLOCKS, TILE, KB), F32),
            pltpu.VMEM((TILE, HD), F32),
            pltpu.VMEM((TILE, 10 * HD), F32),
            pltpu.VMEM((P_SIZE * TILE, HD), F32),
            pltpu.VMEM(OUT, BF16),
            pltpu.SemaphoreType.DMA((2, SPANS)),
            pltpu.SemaphoreType.DMA((2,)),
        ],
        compiler_params=pltpu.CompilerParams(vmem_limit_bytes=LIMIT * 2**20),
        cost_estimate=pl.CostEstimate(flops=flops, transcendentals=0, bytes_accessed=8 * 2**20),
        name="attend",
    )(meta, x, *pieces)


def place(part, part_ref, *refs):
    primal_ref, tangent_ref, sems = refs[-3:]
    rows = pl.ds(part * TOKENS, TOKENS)
    copies = []
    for g in range(ULY):
        copies.append((part_ref.at[g, :, 1:], tangent_ref.at[rows, g]))
        copies.append((part_ref.at[g, :, 0], primal_ref.at[rows, g]))
    copies = [pltpu.make_async_copy(a, b, sems.at[n]) for n, (a, b) in enumerate(copies)]
    for copy in copies:
        copy.start()
    for copy in copies:
        copy.wait()


def assemble(parts):
    placed = ()
    for n, part in enumerate(parts):
        placed = pl.pallas_call(
            functools.partial(place, n),
            out_shape=(
                jax.ShapeDtypeStruct((ROWS, ULY, GROUP, HD), BF16),
                jax.ShapeDtypeStruct((ROWS, ULY, P_SIZE, GROUP, HD), BF16),
            ),
            in_specs=[pl.BlockSpec(memory_space=pltpu.VMEM)]
            + [pl.BlockSpec(memory_space=pltpu.HBM)] * len(placed),
            out_specs=(pl.BlockSpec(memory_space=pltpu.HBM),) * 2,
            scratch_shapes=[pltpu.SemaphoreType.DMA((2 * ULY,))],
            input_output_aliases={1 + k: k for k in range(len(placed))},
            compiler_params=pltpu.CompilerParams(vmem_limit_bytes=8 * 2**20),
            name="place",
        )(part, *placed)
    return placed


def gather_blocks(here):
    up = [(i, (i + 1) % 4) for i in range(4)]
    down = [(i, (i + 3) % 4) for i in range(4)]
    below = lax.ppermute(here, "z", up)
    above = lax.ppermute(here, "z", down)
    far_low = lax.ppermute(below[: 2 * SPAN], "z", up)
    far_high = lax.ppermute(above[2 * SPAN :], "z", down)
    mine = [here, below, above, far_low, far_high]
    return mine + [lax.ppermute(a, "core", [(0, 1), (1, 0)]) for a in mine]


def per_device(queries, query_tangents, keys, key_tangents, values, value_tangents, span_order):
    packed = jnp.concatenate(
        [
            keys.reshape(ROWS, KVH, HD),
            key_tangents.reshape(ROWS, KVH, P_SIZE * HD),
            values.reshape(ROWS, KVH, HD),
            value_tangents.reshape(ROWS, KVH, P_SIZE * HD),
        ],
        axis=2,
    )
    heads = ("y", "xl")
    packed = jnp.broadcast_to(packed[:, None], (ROWS, 2, KVH, WIDTH))
    packed = packed.reshape(ROWS, 2 * KVH, WIDTH).transpose(1, 0, 2)
    head_kv = lax.all_to_all(packed, ("xh",) + heads, 0, 0, tiled=True)
    pieces = gather_blocks(head_kv.reshape(2 * ULY * ROWS, WIDTH))

    q = queries.reshape(ROWS, ULY, GROUP, HD).transpose(1, 0, 2, 3)
    qt = query_tangents.reshape(ROWS, ULY, GROUP, P_SIZE, HD).transpose(1, 3, 0, 2, 4)
    blk = lax.axis_index(("z", "xh", "core")).astype(jnp.int32)
    meta = jnp.concatenate([span_order, blk[None]])
    x = jnp.concatenate(
        [
            q.reshape(ULY, 1, ROWS * GROUP, HD),
            qt.reshape(ULY, P_SIZE, ROWS * GROUP, HD),
        ],
        axis=1,
    )
    x = lax.all_to_all(x, heads, 0, 0, tiled=True)
    sent = []
    for part in range(PARTS):
        out = attention(meta, x, pieces, part)
        sent.append(lax.all_to_all(out, heads, 0, 0, tiled=True))
    primal, tangent = assemble(sent)
    return primal.reshape(ROWS, HQ, HD), tangent.reshape(ROWS, HQ, P_SIZE, HD)


def solution(mesh):
    grid = Mesh(mesh.devices.reshape(4, 2, 2, 4, 2), AXES)
    rows = P(AXES)
    return jax.shard_map(
        per_device,
        mesh=grid,
        in_specs=(rows,) * 6 + (P(),),
        out_specs=(rows, rows),
        check_vma=False,
    )
```
